32 devices in a mesh: patch: 8 (over y, x, core), tensor: 4 (over z).
Axes of the slice: x: 2, y: 2, z: 4, core: 2. Of those that a mesh axis runs over, the one named last changes fastest.
Arguments:
- tokens: bfloat16 [8192, 3072], P(('patch', 'tensor')), may hold values from -6 to 6
- text_tokens: bfloat16 [512, 3072], P('patch'), may hold values from -6 to 6
- img_shift: float32 [3072], replicated, may hold values from -3 to 3
- img_scale: float32 [3072], replicated, may hold values from -3 to 3
- img_gate: float32 [3072], replicated, may hold values from 0.5 to 2
- txt_shift: float32 [3072], replicated, may hold values from -3 to 3
- txt_scale: float32 [3072], replicated, may hold values from -3 to 3
- qkv_weight: bfloat16 [3072, 3, 2048], P(None, None, 'tensor'), may hold values from -0.109375 to 0.109375
- txt_kv_weight: bfloat16 [3072, 2, 2048], P(None, None, 'tensor'), may hold values from -0.109375 to 0.109375
- q_gain: float32 [128], replicated, may hold values from 1 to 3
- k_gain: float32 [128], replicated, may hold values from 1 to 3
- txt_k_gain: float32 [128], replicated, may hold values from 1 to 3
- out_weight: bfloat16 [2048, 3072], P('tensor'), may hold values from -0.125 to 0.125
- stale_keys: bfloat16 [8192, 2048], P('patch', 'tensor'), may hold values from -600 to 600
- stale_values: bfloat16 [8192, 2048], P('patch', 'tensor'), may hold values from -6 to 6
Outputs:
- updated: bfloat16 [8192, 3072], P(('patch', 'tensor'))
- new_keys: bfloat16 [8192, 2048], P('patch', 'tensor')
- new_values: bfloat16 [8192, 2048], P('patch', 'tensor')
The draws below stay inside these ranges and needn't reach their ends.
All inputs are finite; a program needn't handle non-finite values.
Results may differ from the reference program's by a relative error of at most 0.015.
The reference program's roundings to bfloat16 on the way (of `image_mod`, `text_mod` and `attended`) count: a program that leaves them out, or rounds other values in their place, can miss the bound.
Values may be sent and summed in bfloat16 or wider, within the bound.
No kernel may reach another device: no remote copies, remote signals or barrier semaphores. Data moves between devices by JAX's collectives and lax.ppermute only.
A program may use at most 320 MiB of HBM per device.

```python
import math
import jax
import jax.numpy as jnp
from jax import lax

D = 3072
HD = 128
HEADS = 16
ROWS = 1024
TXT = 512
IMG = 8192
N_PATCH = 8


def draw_stale_keys(key, part):
    first = jax.random.fold_in(key, 0)
    base = jnp.clip(2.0 * jax.random.normal(first, (IMG, HEADS * HD), jnp.float32), -12.0, 12.0)
    return base.astype(jnp.bfloat16)


def block_levels(rng, dims, shards, smallest, high):
    def one(dim, blocks):
        steps = jax.random.uniform(jax.random.fold_in(jax.random.fold_in(rng, 6), dim), (blocks,), jnp.float32, smallest / len(shards), high / len(shards))
        return jnp.repeat(jnp.exp(steps), dims[dim] // blocks).reshape((-1,) + (1,) * (len(dims) - dim - 1))

    loudness = one(*shards[0])
    for cut in shards[1:]:
        loudness = loudness * one(*cut)
    return loudness


def scatter_about(rng, shape, deviation, reach, cuts=(), kind=jnp.bfloat16):
    level = block_levels(rng, shape, cuts, -0.22, 0.18) if cuts else 1.0
    result = jax.random.normal(rng, shape, jnp.float32) * deviation * level
    return jnp.minimum(jnp.maximum(result, -reach), reach).astype(kind)


def setup_inputs(seed: int = 0) -> dict:
    keys = jax.random.split(jax.random.key(seed), 16)
    tokens = scatter_about(keys[0], (IMG, D), 1.0, 6.0, ((0, 32),))
    text_tokens = scatter_about(keys[1], (TXT, D), 1.0, 6.0, ((0, 8),))
    img_shift = scatter_about(keys[2], (D,), 0.5, 3.0, (), jnp.float32)
    img_scale = scatter_about(keys[3], (D,), 0.5, 3.0, (), jnp.float32)
    img_gate = jnp.clip(jax.random.uniform(keys[4], (D,), jnp.float32, 0.5, 2.0), 0.5, 2.0)
    txt_shift = scatter_about(keys[5], (D,), 0.5, 3.0, (), jnp.float32)
    txt_scale = scatter_about(keys[6], (D,), 0.5, 3.0, (), jnp.float32)
    qkv_weight = scatter_about(keys[7], (D, 3, HEADS * HD), D ** -0.5, 0.109375, ((2, 4),))
    txt_kv_weight = scatter_about(keys[8], (D, 2, HEADS * HD), D ** -0.5, 0.109375, ((2, 4),))
    q_gain = jnp.clip(jnp.exp(jax.random.uniform(keys[9], (HD,), jnp.float32, math.log(1.0), math.log(3.0))), 1.0, 3.0)
    k_gain = jnp.clip(jnp.exp(jax.random.uniform(keys[10], (HD,), jnp.float32, math.log(1.0), math.log(3.0))), 1.0, 3.0)
    txt_k_gain = jnp.clip(jnp.exp(jax.random.uniform(keys[11], (HD,), jnp.float32, math.log(1.0), math.log(3.0))), 1.0, 3.0)
    out_weight = scatter_about(keys[12], (HEADS * HD, D), (HEADS * HD) ** -0.5, 0.125, ((0, 4),))
    stale_keys = draw_stale_keys(jax.random.fold_in(keys[15], 71), 0)
    stale_values = scatter_about(keys[14], (IMG, HEADS * HD), 1.0, 6.0, ((0, 8), (1, 4)))
    return dict(tokens=tokens, text_tokens=text_tokens, img_shift=img_shift, img_scale=img_scale, img_gate=img_gate, txt_shift=txt_shift, txt_scale=txt_scale, qkv_weight=qkv_weight, txt_kv_weight=txt_kv_weight, q_gain=q_gain, k_gain=k_gain, txt_k_gain=txt_k_gain, out_weight=out_weight, stale_keys=stale_keys, stale_values=stale_values)


def layer_mod(values, shift_vec, scale_vec):
    wide = values.astype(jnp.float32)
    centre = lax.optimization_barrier(jnp.mean(wide, axis=-1, keepdims=True))
    spread = lax.optimization_barrier(jnp.mean((wide - centre) * (wide - centre), axis=-1, keepdims=True))
    normed = (wide - centre) * lax.rsqrt(spread + 1e-06)
    return ((1.0 + scale_vec) * normed + shift_vec).astype(jnp.bfloat16)

def rms_gain(values, gain_vec):
    square = lax.optimization_barrier(jnp.mean(values * values, axis=-1, keepdims=True))
    return values * lax.rsqrt(square + 1e-06) * gain_vec

def reference(tokens, text_tokens, img_shift, img_scale, img_gate, txt_shift, txt_scale, qkv_weight, txt_kv_weight, q_gain, k_gain, txt_k_gain, out_weight, stale_keys, stale_values):
    image_mod = layer_mod(tokens, img_shift, img_scale)
    projected = jnp.dot(image_mod, qkv_weight.reshape(D, 3 * HEADS * HD), preferred_element_type=jnp.float32)
    projected = projected.reshape(IMG, 3, HEADS, HD)
    queries = rms_gain(projected[:, 0], q_gain).astype(jnp.bfloat16)
    fresh_keys = rms_gain(projected[:, 1], k_gain).astype(jnp.bfloat16)
    fresh_values = projected[:, 2].astype(jnp.bfloat16)
    text_mod = layer_mod(text_tokens, txt_shift, txt_scale)
    text_proj = jnp.dot(text_mod, txt_kv_weight.reshape(D, 2 * HEADS * HD), preferred_element_type=jnp.float32)
    text_proj = text_proj.reshape(TXT, 2, HEADS, HD)
    text_keys = rms_gain(text_proj[:, 0], txt_k_gain).astype(jnp.bfloat16)
    text_values = text_proj[:, 1].astype(jnp.bfloat16)
    old_keys = stale_keys.reshape(IMG, HEADS, HD)
    old_values = stale_values.reshape(IMG, HEADS, HD)
    factor = 1.0 / math_sqrt(HD)
    zero = jnp.int32(0)

    def one_patch(patch_idx):
        offset = (patch_idx * ROWS).astype(jnp.int32)
        own_keys = lax.dynamic_slice_in_dim(fresh_keys, offset, ROWS, 0)
        own_values = lax.dynamic_slice_in_dim(fresh_values, offset, ROWS, 0)
        key_rows = lax.dynamic_update_slice(old_keys, own_keys, (offset, zero, zero))
        value_rows = lax.dynamic_update_slice(old_values, own_values, (offset, zero, zero))
        key_rows = jnp.concatenate([key_rows, text_keys], axis=0)
        value_rows = jnp.concatenate([value_rows, text_values], axis=0)
        query_rows = lax.dynamic_slice_in_dim(queries, offset, ROWS, 0)
        scores = jnp.einsum('qhd,khd->hqk', query_rows.astype(jnp.float32), key_rows.astype(jnp.float32)) * factor
        highest = lax.optimization_barrier(jnp.max(scores, axis=-1, keepdims=True))
        weights = jnp.exp(scores - highest)
        denominator = lax.optimization_barrier(jnp.sum(weights, axis=-1))
        rounded = weights.astype(jnp.bfloat16).astype(jnp.float32)
        numerator = jnp.einsum('hqk,khd->qhd', rounded, value_rows.astype(jnp.float32))
        return (numerator / jnp.transpose(denominator)[:, :, None]).astype(jnp.bfloat16)
    attended = lax.map(one_patch, jnp.arange(N_PATCH, dtype=jnp.int32)).reshape(IMG, HEADS * HD)
    branch = jnp.dot(attended, out_weight, preferred_element_type=jnp.float32)
    updated = (tokens.astype(jnp.float32) + img_gate * branch).astype(jnp.bfloat16)
    return (updated, fresh_keys.reshape(IMG, HEADS * HD), fresh_values.reshape(IMG, HEADS * HD))

def math_sqrt(number):
    return float(number) ** 0.5
```

```python
from functools import partial

import jax
import jax.numpy as jnp
from jax import lax
from jax.experimental import pallas as pl
from jax.experimental.pallas import tpu as pltpu
from jax.sharding import PartitionSpec as P


def layer_mod(values, shift_vec, scale_vec):
    wide = values.astype(jnp.float32)
    centre = jnp.mean(wide, axis=-1, keepdims=True)
    spread = jnp.mean((wide - centre) * (wide - centre), axis=-1, keepdims=True)
    normed = (wide - centre) * lax.rsqrt(spread + 1e-06)
    return ((1.0 + scale_vec) * normed + shift_vec).astype(jnp.bfloat16)


def rms_gain(values, gain_vec):
    square = jnp.mean(values * values, axis=-1, keepdims=True)
    return values * lax.rsqrt(square + 1e-06) * gain_vec


def attend_body(own_ref, q_ref, fk_ref, fv_ref, tk_ref, tv_ref, sk_ref, sv_ref, o_ref, m_ref, l_ref, acc_ref, *, unit, skip, block, factor):
    rows = q_ref.shape[0]
    m_ref[...] = jnp.full(m_ref.shape, -1e30, jnp.float32)
    l_ref[...] = jnp.zeros(l_ref.shape, jnp.float32)
    acc_ref[...] = jnp.zeros(acc_ref.shape, jnp.float32)

    def absorb(key_rows, value_rows):
        for first in range(0, rows, unit):
            cols = pl.ds(first, unit)
            scores = factor * lax.dot_general(
                key_rows, q_ref[cols, :], (((1,), (1,)), ((), ())), preferred_element_type=jnp.float32
            )
            old_peak = m_ref[:, cols]
            peak = jnp.maximum(old_peak, jnp.max(scores, axis=0, keepdims=True))
            weights = jnp.exp2(scores - peak)
            rescale = jnp.exp2(old_peak - peak)
            m_ref[:, cols] = peak
            l_ref[:, cols] = l_ref[:, cols] * rescale + jnp.sum(weights, axis=0, keepdims=True)
            acc_ref[:, cols] = acc_ref[:, cols] * rescale + lax.dot_general(
                value_rows, weights.astype(jnp.bfloat16), (((0,), (0,)), ((), ())),
                preferred_element_type=jnp.float32,
            )

    def sweep(k_ref, v_ref, jump):
        def step(i, carry):
            start = i * block
            if jump:
                start = start + jnp.where(start >= own_ref[0], skip, 0)
            start = pl.multiple_of(start, block)
            absorb(k_ref[pl.ds(start, block), :], v_ref[pl.ds(start, block), :])
            return carry

        total = k_ref.shape[0] - (skip if jump else 0)
        lax.fori_loop(0, total // block, step, 0)

    sweep(fk_ref, fv_ref, False)
    sweep(tk_ref, tv_ref, False)
    sweep(sk_ref, sv_ref, True)
    o_ref[...] = jnp.transpose(acc_ref[...] / l_ref[...]).astype(jnp.bfloat16)


def attend(own, queries, fk, fv, tk, tv, sk, sv, head_dim):
    rows, feats = queries.shape
    heads = feats // head_dim
    unit = 256 if rows % 256 == 0 else rows
    skip = fk.shape[0]
    block = 512
    for other in (skip, tk.shape[0], sk.shape[0]):
        while other % block:
            block //= 2
    keys = fk.shape[0] + tk.shape[0] + sk.shape[0] - skip
    factor = 1.4426950408889634 / float(head_dim) ** 0.5

    def column(values):
        return pl.BlockSpec((values.shape[0], head_dim), lambda h, own_ref: (0, h))

    def kernel(*refs):
        attend_body(*refs, unit=unit, skip=skip, block=block, factor=factor)

    return pl.pallas_call(
        kernel,
        out_shape=jax.ShapeDtypeStruct((rows, feats), jnp.bfloat16),
        grid_spec=pltpu.PrefetchScalarGridSpec(
            num_scalar_prefetch=1,
            grid=(heads,),
            in_specs=[column(a) for a in (queries, fk, fv, tk, tv, sk, sv)],
            out_specs=column(queries),
            scratch_shapes=[
                pltpu.VMEM((1, rows), jnp.float32),
                pltpu.VMEM((1, rows), jnp.float32),
                pltpu.VMEM((head_dim, rows), jnp.float32),
            ],
        ),
        cost_estimate=pl.CostEstimate(
            flops=4 * rows * keys * feats,
            transcendentals=rows * keys * heads,
            bytes_accessed=4 * (keys + rows) * feats,
        ),
        name="attend",
    )(own, queries, fk, fv, tk, tv, sk, sv)


def per_device(
    tokens, text_tokens, img_shift, img_scale, img_gate, txt_shift, txt_scale, qkv_weight,
    txt_kv_weight, q_gain, k_gain, txt_k_gain, out_weight, stale_keys, stale_values, *, n_patch, n_tensor
):
    width = tokens.shape[1]
    head_dim = q_gain.shape[0]
    feats = qkv_weight.shape[2]
    local_heads = feats // head_dim
    here = lax.axis_index("tensor")
    place = lax.axis_index("patch")
    rows = tokens.shape[0]
    patch_rows = rows * n_tensor
    ahead = [(i, (i + 1) % n_tensor) for i in range(n_tensor)]
    back = [(i, (i - 1) % n_tensor) for i in range(n_tensor)]

    def normed(values, gain_vec):
        split = values.reshape(values.shape[0], local_heads, head_dim)
        return rms_gain(split, gain_vec).astype(jnp.bfloat16).reshape(values.shape)

    key_rows = lax.all_gather(stale_keys, "patch", axis=0, tiled=True)

    image_mods = [layer_mod(tokens, img_shift, img_scale)]
    for _ in range(1, n_tensor):
        image_mods.append(lax.ppermute(image_mods[-1], "tensor", ahead))
    portion = out_weight.shape[0] // n_patch
    moving = lax.dynamic_slice_in_dim(out_weight, place * portion, portion, 0)
    weight_parts = []
    for _ in range(1, n_tensor):
        moving = lax.ppermute(moving, "tensor", back)
        weight_parts.append(moving)

    text_mod = layer_mod(text_tokens, txt_shift, txt_scale)
    text_proj = jnp.dot(
        text_mod, txt_kv_weight.reshape(width, 2 * feats), preferred_element_type=jnp.float32
    )
    text_pairs = jnp.concatenate(
        [normed(text_proj[:, :feats], txt_k_gain), text_proj[:, feats:].astype(jnp.bfloat16)], axis=1
    )
    all_text = lax.all_gather(text_pairs, "patch", axis=0, tiled=True)
    stale_values, all_text = lax.optimization_barrier((stale_values, all_text))
    value_rows = lax.all_gather(stale_values, "patch", axis=0, tiled=True)
    weight_parts, value_rows = lax.optimization_barrier((weight_parts, value_rows))
    weights = [out_weight] + [lax.all_gather(w, "patch", axis=0, tiled=True) for w in weight_parts]

    flat_weight = qkv_weight.reshape(width, 3 * feats)
    queries, fresh_keys, fresh_values = [], [], []
    new_keys = jnp.zeros((patch_rows, feats), jnp.bfloat16)
    new_values = jnp.zeros((patch_rows, feats), jnp.bfloat16)
    for s in range(n_tensor):
        projected = jnp.dot(image_mods[s], flat_weight, preferred_element_type=jnp.float32)
        queries.append(normed(projected[:, :feats], q_gain))
        fresh_keys.append(normed(projected[:, feats : 2 * feats], k_gain))
        fresh_values.append(projected[:, 2 * feats :].astype(jnp.bfloat16))
        at = ((here - s) % n_tensor) * rows
        new_keys = lax.dynamic_update_slice_in_dim(new_keys, fresh_keys[s], at, 0)
        new_values = lax.dynamic_update_slice_in_dim(new_values, fresh_values[s], at, 0)

    own = jnp.reshape(place * patch_rows, (1,)).astype(jnp.int32)
    shared = (new_keys, new_values, all_text[:, :feats], all_text[:, feats:], key_rows, value_rows)
    others = attend(own, jnp.concatenate(queries[1:], axis=0), *shared, head_dim)
    received = []
    for s in range(1, n_tensor):
        to = [(i, (i - s) % n_tensor) for i in range(n_tensor)]
        received.append(lax.ppermute(others[(s - 1) * rows : s * rows], "tensor", to))
    received.insert(0, attend(own, queries[0], *shared, head_dim))
    branch = jnp.zeros((rows, width), jnp.float32)
    for s in range(n_tensor):
        branch = branch + jnp.dot(received[s], weights[s], preferred_element_type=jnp.float32)
    updated = (tokens.astype(jnp.float32) + img_gate * branch).astype(jnp.bfloat16)
    return (updated, new_keys, new_values)


def solution(mesh):
    placed = (
        P(("patch", "tensor"), None),
        P("patch", None),
        P(),
        P(),
        P(),
        P(),
        P(),
        P(None, None, "tensor"),
        P(None, None, "tensor"),
        P(),
        P(),
        P(),
        P("tensor", None),
        P("patch", "tensor"),
        P("patch", "tensor"),
    )
    return jax.shard_map(
        partial(per_device, n_patch=mesh.shape["patch"], n_tensor=mesh.shape["tensor"]),
        mesh=mesh,
        in_specs=placed,
        out_specs=(P(("patch", "tensor"), None), P("patch", "tensor"), P("patch", "tensor")),
        check_vma=False,
    )
```

```python
from functools import partial

import jax
import jax.numpy as jnp
from jax import lax
from jax.experimental import pallas as pl
from jax.experimental.pallas import tpu as pltpu
from jax.sharding import PartitionSpec as P


def layer_mod(values, shift_vec, scale_vec):
    wide = values.astype(jnp.float32)
    centre = jnp.mean(wide, axis=-1, keepdims=True)
    spread = jnp.mean((wide - centre) * (wide - centre), axis=-1, keepdims=True)
    normed = (wide - centre) * lax.rsqrt(spread + 1e-06)
    return ((1.0 + scale_vec) * normed + shift_vec).astype(jnp.bfloat16)


def rms_gain(values, gain_vec):
    square = jnp.mean(values * values, axis=-1, keepdims=True)
    return values * lax.rsqrt(square + 1e-06) * gain_vec


def attend_body(own_ref, q_ref, fk_ref, fv_ref, tk_ref, tv_ref, sk_ref, sv_ref, o_ref, m_ref, l_ref, acc_ref, *, unit, skip, block, factor):
    rows = q_ref.shape[0]
    m_ref[...] = jnp.full(m_ref.shape, -1e30, jnp.float32)
    l_ref[...] = jnp.zeros(l_ref.shape, jnp.float32)
    acc_ref[...] = jnp.zeros(acc_ref.shape, jnp.float32)

    def score(k_ref, at, first):
        return factor * lax.dot_general(
            k_ref[pl.ds(at, block), :], q_ref[pl.ds(first, unit), :],
            (((1,), (1,)), ((), ())), preferred_element_type=jnp.float32,
        )

    def absorb(scores, v_ref, at, first):
        cols = pl.ds(first, unit)
        old_peak = m_ref[:, cols]
        peak = jnp.maximum(old_peak, jnp.max(scores, axis=0, keepdims=True))
        weights = jnp.exp2(scores - peak)
        rescale = jnp.exp2(old_peak - peak)
        m_ref[:, cols] = peak
        l_ref[:, cols] = l_ref[:, cols] * rescale + jnp.sum(weights, axis=0, keepdims=True)
        acc_ref[:, cols] = acc_ref[:, cols] * rescale + lax.dot_general(
            v_ref[pl.ds(at, block), :], weights.astype(jnp.bfloat16),
            (((0,), (0,)), ((), ())), preferred_element_type=jnp.float32,
        )

    def sweep(k_ref, v_ref, jump):
        total = k_ref.shape[0] - (skip if jump else 0)
        pieces = 2 if total % (2 * block) == 0 and skip % (2 * block) == 0 else 1
        stride = pieces * block

        def step(i, carry):
            start = i * stride
            if jump:
                start = start + jnp.where(start >= own_ref[0], skip, 0)
            start = pl.multiple_of(start, stride)
            items = [(start + p * block, f) for p in range(pieces) for f in range(0, rows, unit)]
            ready = score(k_ref, *items[0])
            for n, item in enumerate(items):
                scores = ready
                if n + 1 < len(items):
                    ready = score(k_ref, *items[n + 1])
                absorb(scores, v_ref, *item)
            return carry

        lax.fori_loop(0, total // stride, step, 0)

    sweep(fk_ref, fv_ref, False)
    sweep(tk_ref, tv_ref, False)
    sweep(sk_ref, sv_ref, True)
    o_ref[...] = jnp.transpose(acc_ref[...] / l_ref[...]).astype(jnp.bfloat16)


def attend(own, queries, fk, fv, tk, tv, sk, sv, head_dim):
    rows, feats = queries.shape
    heads = feats // head_dim
    unit = 256 if rows % 256 == 0 else rows
    skip = fk.shape[0]
    block = 512
    for other in (skip, tk.shape[0], sk.shape[0]):
        while other % block:
            block //= 2
    keys = fk.shape[0] + tk.shape[0] + sk.shape[0] - skip
    factor = 1.4426950408889634 / float(head_dim) ** 0.5

    def column(values):
        return pl.BlockSpec((values.shape[0], head_dim), lambda h, own_ref: (0, h))

    def kernel(*refs):
        attend_body(*refs, unit=unit, skip=skip, block=block, factor=factor)

    return pl.pallas_call(
        kernel,
        out_shape=jax.ShapeDtypeStruct((rows, feats), jnp.bfloat16),
        grid_spec=pltpu.PrefetchScalarGridSpec(
            num_scalar_prefetch=1,
            grid=(heads,),
            in_specs=[column(a) for a in (queries, fk, fv, tk, tv, sk, sv)],
            out_specs=column(queries),
            scratch_shapes=[
                pltpu.VMEM((1, rows), jnp.float32),
                pltpu.VMEM((1, rows), jnp.float32),
                pltpu.VMEM((head_dim, rows), jnp.float32),
            ],
        ),
        cost_estimate=pl.CostEstimate(
            flops=4 * rows * keys * feats,
            transcendentals=rows * keys * heads,
            bytes_accessed=4 * (keys + rows) * feats,
        ),
        name="attend",
    )(own, queries, fk, fv, tk, tv, sk, sv)


def per_device(
    tokens, text_tokens, img_shift, img_scale, img_gate, txt_shift, txt_scale, qkv_weight,
    txt_kv_weight, q_gain, k_gain, txt_k_gain, out_weight, stale_keys, stale_values, *, n_patch, n_tensor
):
    width = tokens.shape[1]
    head_dim = q_gain.shape[0]
    feats = qkv_weight.shape[2]
    local_heads = feats // head_dim
    here = lax.axis_index("tensor")
    place = lax.axis_index("patch")
    rows = tokens.shape[0]
    patch_rows = rows * n_tensor
    ahead = [(i, (i + 1) % n_tensor) for i in range(n_tensor)]
    back = [(i, (i - 1) % n_tensor) for i in range(n_tensor)]

    def normed(values, gain_vec):
        split = values.reshape(values.shape[0], local_heads, head_dim)
        return rms_gain(split, gain_vec).astype(jnp.bfloat16).reshape(values.shape)

    key_rows = lax.all_gather(stale_keys, "patch", axis=0, tiled=True)

    image_mods = [layer_mod(tokens, img_shift, img_scale)]
    text_tokens, image_mods[0] = lax.optimization_barrier((text_tokens, image_mods[0]))
    flat_weight = qkv_weight.reshape(width, 3 * feats)
    queries, fresh_keys, fresh_values = [], [], []
    for s in range(n_tensor):
        if s + 1 < n_tensor:
            sent = image_mods[s]
            if s:
                sent, queries[-1], fresh_keys[-1] = lax.optimization_barrier(
                    (sent, queries[-1], fresh_keys[-1])
                )
            image_mods.append(lax.ppermute(sent, "tensor", ahead))
        projected = jnp.dot(image_mods[s], flat_weight, preferred_element_type=jnp.float32)
        queries.append(normed(projected[:, :feats], q_gain))
        fresh_keys.append(normed(projected[:, feats : 2 * feats], k_gain))
        fresh_values.append(projected[:, 2 * feats :].astype(jnp.bfloat16))
    portion = out_weight.shape[0] // n_patch
    moving = lax.dynamic_slice_in_dim(out_weight, place * portion, portion, 0)
    moving, image_mods[-1] = lax.optimization_barrier((moving, image_mods[-1]))
    weight_parts = []
    for _ in range(1, n_tensor):
        moving = lax.ppermute(moving, "tensor", back)
        weight_parts.append(moving)

    text_mod = layer_mod(text_tokens, txt_shift, txt_scale)
    text_proj = jnp.dot(
        text_mod, txt_kv_weight.reshape(width, 2 * feats), preferred_element_type=jnp.float32
    )
    text_pairs = jnp.concatenate(
        [normed(text_proj[:, :feats], txt_k_gain), text_proj[:, feats:].astype(jnp.bfloat16)], axis=1
    )
    all_text = lax.all_gather(text_pairs, "patch", axis=0, tiled=True)
    stale_values, all_text = lax.optimization_barrier((stale_values, all_text))
    value_rows = lax.all_gather(stale_values, "patch", axis=0, tiled=True)
    weights = [out_weight] + [lax.all_gather(w, "patch", axis=0, tiled=True) for w in weight_parts]

    new_keys = jnp.zeros((patch_rows, feats), jnp.bfloat16)
    new_values = jnp.zeros((patch_rows, feats), jnp.bfloat16)
    for s in range(n_tensor):
        at = ((here - s) % n_tensor) * rows
        new_keys = lax.dynamic_update_slice_in_dim(new_keys, fresh_keys[s], at, 0)
        new_values = lax.dynamic_update_slice_in_dim(new_values, fresh_values[s], at, 0)

    own = jnp.reshape(place * patch_rows, (1,)).astype(jnp.int32)
    shared = (new_keys, new_values, all_text[:, :feats], all_text[:, feats:], key_rows, value_rows)
    others = attend(own, jnp.concatenate(queries[1:], axis=0), *shared, head_dim)
    received = []
    for s in range(1, n_tensor):
        to = [(i, (i - s) % n_tensor) for i in range(n_tensor)]
        received.append(lax.ppermute(others[(s - 1) * rows : s * rows], "tensor", to))
    received.insert(0, attend(own, queries[0], *shared, head_dim))
    branch = jnp.zeros((rows, width), jnp.float32)
    for s in range(n_tensor):
        branch = branch + jnp.dot(received[s], weights[s], preferred_element_type=jnp.float32)
    updated = (tokens.astype(jnp.float32) + img_gate * branch).astype(jnp.bfloat16)
    return (updated, new_keys, new_values)


def solution(mesh):
    placed = (
        P(("patch", "tensor"), None),
        P("patch", None),
        P(),
        P(),
        P(),
        P(),
        P(),
        P(None, None, "tensor"),
        P(None, None, "tensor"),
        P(),
        P(),
        P(),
        P("tensor", None),
        P("patch", "tensor"),
        P("patch", "tensor"),
    )
    return jax.shard_map(
        partial(per_device, n_patch=mesh.shape["patch"], n_tensor=mesh.shape["tensor"]),
        mesh=mesh,
        in_specs=placed,
        out_specs=(P(("patch", "tensor"), None), P("patch", "tensor"), P("patch", "tensor")),
        check_vma=False,
    )
```
